32 devices in a mesh: group: 8 (over y, x, core), shard: 4 (over z).
Axes of the slice: x: 2, y: 2, z: 4, core: 2. Of those that a mesh axis runs over, the one named last changes fastest.
Arguments:
- momentum: bfloat16 [8, 7168, 2048], P(None, ('group', 'shard'))
- gradient: bfloat16 [8, 7168, 2048], P(None, ('group', 'shard'))
- q_prev: bfloat16 [8, 3, 2048, 128], P('group', None, 'shard'), may hold values from -6 to 6
- owner_group: int32 [8], replicated, may hold values from 0 to 7, as said below
- group_counts: int32 [8], replicated, may hold values from 0 to 3, as said below
Outputs:
- momentum_next: bfloat16 [8, 7168, 2048], P(None, ('group', 'shard'))
- update: bfloat16 [8, 7168, 2048], P(None, ('group', 'shard'))
- q_next: bfloat16 [8, 3, 2048, 128], P('group', None, 'shard')
The draws below stay inside these ranges and needn't reach their ends.
Inputs may be any that keep to these rules, and one draw needn't show every extreme that they name: `owner_group`: each group owns at most 3 experts and some group owns exactly 3; a group's experts fill its slots 0, 1, ... in increasing expert order. `group_counts`: entry g is the number of experts whose owner_group is g, except for one or two groups that own some experts, where it is one less; it equals 3 for some group that owns 3 experts.
All inputs are finite; a program needn't handle non-finite values.
Results may differ from the reference program's by a relative error of at most 0.0059.
Values may be sent and summed in bfloat16 or wider, within the bound.
A program may use at most 128 MiB of HBM per device.

```python
import math
import jax
import jax.numpy as jnp
from jax import lax

D = 7168
H = 2048
RANK = 128
EXPERTS = 8
CAP = 3
BLOCK = 224
N_GROUP = 8
N_SHARD = 4


def entry_scales(key):
    rows = jnp.arange(D, dtype=jnp.int32)
    position = (rows // BLOCK % N_SHARD).astype(jnp.float32) / max(N_SHARD - 1, 1)
    rising = jnp.exp(math.log(3.0) * (position - 0.5))
    row_scale = jnp.exp(jax.random.uniform(jax.random.fold_in(key, 21), (EXPERTS, D, 1), jnp.float32, math.log(0.3), math.log(3.0)))
    col_scale = jnp.exp(jax.random.uniform(jax.random.fold_in(key, 22), (EXPERTS, 1, H), jnp.float32, math.log(0.3), math.log(3.0)))
    return row_scale * rising[None, :, None] * col_scale


def shared_part(key):
    left_factor = jax.random.normal(jax.random.fold_in(key, 41), (EXPERTS, D, RANK), jnp.float32)
    right_factor = jax.random.normal(jax.random.fold_in(key, 42), (EXPERTS, RANK, H), jnp.float32)
    return jnp.einsum('edk,ekh->edh', left_factor, right_factor) / math.sqrt(RANK)


def noise_part(key, salt):
    base = jax.random.fold_in(key, salt)
    values = jax.random.normal(base, (EXPERTS, D, H), jnp.float32)
    return values


def entries(key, salt):
    mixed = 0.894 * shared_part(key) + 0.447 * noise_part(key, salt)
    return mixed * entry_scales(key)


def draw_momentum(key, part):
    return entries(key, 31).astype(jnp.bfloat16)


def draw_gradient(key, part):
    return (0.5 * entries(key, 32)).astype(jnp.bfloat16)


def owner_plan(key):
    total_slots = N_GROUP * CAP
    full_group = jax.random.randint(jax.random.fold_in(key, 12), (), 0, N_GROUP)
    slot_ids = jnp.arange(total_slots, dtype=jnp.int32)
    scores = jax.random.randint(jax.random.fold_in(key, 11), (total_slots,), 0, 2 ** 20) * total_slots + slot_ids
    scores = jnp.where(slot_ids // CAP == full_group, scores + 2 ** 30, scores)
    forced_groups = jnp.array([N_GROUP // 2, 0, 3], dtype=jnp.int32)
    forced_slots = forced_groups * CAP
    mandated_reward = jnp.array([2, 1, 0], dtype=jnp.int32)
    mandated_flag = slot_ids[:, None] == forced_slots[None, :]
    mandated_rating = 2 ** 30 + 2 ** 29 + jnp.sum(jnp.where(mandated_flag, mandated_reward[None, :], 0), axis=1)
    scores = jnp.where(jnp.any(mandated_flag, axis=1), mandated_rating, scores).astype(jnp.int32)
    picked_scores, chosen = lax.top_k(scores, EXPERTS)
    chosen_group = (chosen // CAP).astype(jnp.int32)
    shuffle = jax.random.permutation(jax.random.fold_in(key, 13), EXPERTS - 3)
    owner = jnp.concatenate([chosen_group[:3], chosen_group[3:][shuffle]]).astype(jnp.int32)
    group_ids = jnp.arange(N_GROUP, dtype=jnp.int32)
    counts = jnp.sum((owner[None, :] == group_ids[:, None]).astype(jnp.int32), axis=1).astype(jnp.int32)
    holds_forced = jnp.any(group_ids[:, None] == forced_groups[None, :], axis=1)
    eligible = (counts >= 1) & (group_ids != full_group) & jnp.logical_not(holds_forced & (counts < 2))
    group_scores = jax.random.randint(jax.random.fold_in(key, 14), (N_GROUP,), 0, 2 ** 20) * N_GROUP + group_ids
    group_scores = jnp.where(eligible, group_scores + 2 ** 26, group_scores)
    top_scores, picked = lax.top_k(group_scores, 2)
    short = jnp.any(group_ids[:, None] == picked[None, :], axis=1) & eligible
    counts = (counts - short.astype(jnp.int32)).astype(jnp.int32)
    return (owner, counts)


def draw_owner_group(key, part):
    return owner_plan(key)[0]


def draw_group_counts(key, part):
    return owner_plan(key)[1]


def levels(key, dims, split, low, top_value):
    loudness, own = 1.0, jax.random.fold_in(key, 6)
    for axis_at, parts in split:
        heights = jnp.exp(jax.random.uniform(jax.random.fold_in(own, axis_at), (parts,), jnp.float32, low / len(split), top_value / len(split)))
        loudness = loudness * jnp.repeat(heights, dims[axis_at] // parts).reshape([-1 if axis == axis_at else 1 for axis in range(len(dims))])
    return loudness


def gaussian(own_key, shape, deviation, limit, shards=(), kind=jnp.bfloat16):
    gain = levels(own_key, shape, shards, -0.22, 0.18) if shards else 1.0
    values = jax.random.normal(own_key, shape, jnp.float32) * deviation * gain
    return jnp.minimum(jnp.maximum(values, -limit), limit).astype(kind)


def setup_inputs(seed: int = 0) -> dict:
    streams_of = jax.random.split(jax.random.key(seed), 6)
    return {
        "momentum": draw_momentum(jax.random.fold_in(streams_of[5], 71), 0),
        "gradient": draw_gradient(jax.random.fold_in(streams_of[5], 71), 0),
        "q_prev": gaussian(streams_of[2], (N_GROUP, CAP, H, RANK), 1.0, 6.0, ((0, 8), (2, 4))),
        "owner_group": draw_owner_group(jax.random.fold_in(streams_of[5], 71), 0),
        "group_counts": draw_group_counts(jax.random.fold_in(streams_of[5], 71), 0),
    }


stability_offset = 1e-06
momentum_decay = 0.6

def owner_slots(owner_group):
    experts = owner_group.shape[0]
    expert_ids = jnp.arange(experts, dtype=jnp.int32)
    same_owner = owner_group[:, None] == owner_group[None, :]
    earlier = expert_ids[None, :] < expert_ids[:, None]
    return lax.optimization_barrier(jnp.sum((same_owner & earlier).astype(jnp.int32), axis=1)).astype(jnp.int32)

def reference(momentum, gradient, q_prev, owner_group, group_counts):
    slot_of = owner_slots(owner_group)
    keep = slot_of < group_counts[owner_group]
    q_each = q_prev[owner_group, slot_of]
    update_multiplier = math.sqrt(D / RANK)

    def one_expert(items):
        moment_one, grad_one, q_one, keep_one = items
        combined = (moment_one.astype(jnp.float32) + grad_one.astype(jnp.float32)).astype(jnp.bfloat16)
        q_used = jnp.where(keep_one, q_one, jnp.zeros_like(q_one))
        unnormalized_basis = jnp.dot(combined, q_used, preferred_element_type=jnp.float32)
        left_unit = (unnormalized_basis * lax.rsqrt(lax.optimization_barrier(jnp.sum(unnormalized_basis * unnormalized_basis, axis=0)) + stability_offset)[None, :]).astype(jnp.bfloat16)
        right = jnp.dot(combined.T, left_unit, preferred_element_type=jnp.float32)
        q_new = (right * lax.rsqrt(lax.optimization_barrier(jnp.mean(right * right, axis=0)) + stability_offset)[None, :]).astype(jnp.bfloat16)
        update_one = (jnp.dot(left_unit, q_new.T, preferred_element_type=jnp.float32) * update_multiplier).astype(jnp.bfloat16)
        low_rank = jnp.dot(left_unit, right.astype(jnp.bfloat16).T, preferred_element_type=jnp.float32)
        moment_next = (combined.astype(jnp.float32) - (1.0 - momentum_decay) * low_rank).astype(jnp.bfloat16)
        return (moment_next, update_one, jnp.where(keep_one, q_new, jnp.zeros_like(q_new)))
    velocity_states, update_list, q_all = lax.map(one_expert, (momentum, gradient, q_each, keep))
    q_next = jnp.zeros_like(q_prev).at[owner_group, slot_of].set(q_all)
    return (velocity_states, update_list, q_next)
```

```python
import math

import jax
import jax.numpy as jnp
from jax import lax
from jax.sharding import PartitionSpec as P

D = 7168
RANK = 128

stability_offset = 1e-06
momentum_decay = 0.6
AXES = ("group", "shard")


def owner_slots(owner_group):
    experts = owner_group.shape[0]
    expert_ids = jnp.arange(experts, dtype=jnp.int32)
    same_owner = owner_group[:, None] == owner_group[None, :]
    earlier = expert_ids[None, :] < expert_ids[:, None]
    return jnp.sum((same_owner & earlier).astype(jnp.int32), axis=1)


def shards(momentum, gradient, q_prev, owner_group, group_counts):
    me = lax.axis_index("group")
    experts, block, hidden = momentum.shape
    cap, share_rows, rank = q_prev.shape[1:]
    slot_of = owner_slots(owner_group)
    keep = slot_of < group_counts[owner_group]
    mine = keep & (owner_group == me)

    pieces = jnp.zeros((experts, share_rows, rank), jnp.bfloat16)
    for j in range(cap):
        pick = mine & (slot_of == j)
        pieces = jnp.where(pick[:, None, None], q_prev[0, j][None], pieces)
    q_one = lax.psum_scatter(pieces, "group", scatter_dimension=0, tiled=True)
    q_shard = lax.all_gather(q_one, "shard", axis=1, tiled=True)
    q_full = lax.all_gather(q_shard, "group", axis=0, tiled=True)

    combined = (momentum.astype(jnp.float32) + gradient.astype(jnp.float32)).astype(jnp.bfloat16)
    left_raw = jnp.einsum("erh,ehk->erk", combined, q_full, preferred_element_type=jnp.float32)
    squares = lax.psum(jnp.sum(left_raw * left_raw, axis=1), AXES)
    left_unit = (left_raw * lax.rsqrt(squares + stability_offset)[:, None, :]).astype(jnp.bfloat16)
    part = jnp.einsum("erh,erk->ehk", combined, left_unit, preferred_element_type=jnp.float32)

    part = lax.psum_scatter(part, "group", scatter_dimension=0, tiled=True)
    share = lax.psum_scatter(part, "shard", scatter_dimension=1, tiled=True)
    right = lax.all_gather(share.astype(jnp.bfloat16), "shard", axis=1, tiled=True)
    right = lax.all_gather(right, "group", axis=0, tiled=True)

    right32 = right.astype(jnp.float32)
    scale = lax.rsqrt(jnp.mean(right32 * right32, axis=1) + stability_offset)
    q_new = (right32 * scale[:, None, :]).astype(jnp.bfloat16)
    update = (
        jnp.einsum("erk,ehk->erh", left_unit, q_new, preferred_element_type=jnp.float32)
        * math.sqrt(D / RANK)
    ).astype(jnp.bfloat16)
    low_rank = jnp.einsum("erk,ehk->erh", left_unit, right, preferred_element_type=jnp.float32)
    momentum_next = (
        combined.astype(jnp.float32) - (1.0 - momentum_decay) * low_rank
    ).astype(jnp.bfloat16)

    rows = lax.dynamic_slice_in_dim(q_new, lax.axis_index("shard") * share_rows, share_rows, axis=1)
    kept = []
    for j in range(cap):
        pick = mine & (slot_of == j)
        kept.append(jnp.sum(jnp.where(pick[:, None, None], rows, jnp.zeros_like(rows)), axis=0))
    return (momentum_next, update, jnp.stack(kept)[None])


def solution(mesh):
    return jax.shard_map(
        shards,
        mesh=mesh,
        in_specs=(
            P(None, AXES, None),
            P(None, AXES, None),
            P("group", None, "shard", None),
            P(),
            P(),
        ),
        out_specs=(P(None, AXES, None), P(None, AXES, None), P("group", None, "shard", None)),
        check_vma=False,
    )
```

```python
import math

import jax
import jax.numpy as jnp
from jax import lax
from jax.experimental import pallas as pl
from jax.experimental.pallas import tpu as pltpu
from jax.sharding import PartitionSpec as P

D = 7168
RANK = 128

stability_offset = 1e-06
momentum_decay = 0.6
AXES = ("group", "shard")


def owner_slots(owner_group):
    experts = owner_group.shape[0]
    expert_ids = jnp.arange(experts, dtype=jnp.int32)
    same_owner = owner_group[:, None] == owner_group[None, :]
    earlier = expert_ids[None, :] < expert_ids[:, None]
    return jnp.sum((same_owner & earlier).astype(jnp.int32), axis=1)


def exchange_sum(x, place, n, split, collective_id):
    rows, cols = x.shape[-2:]
    step = min(rows, 128)

    def kernel(x_ref, o_ref, landed, send_sem, recv_sem):
        me, peer = place()

        def copy(k):
            at = lax.rem(me + k, n)
            return pltpu.make_async_remote_copy(
                src_ref=x_ref.at[at] if split else x_ref,
                dst_ref=landed.at[k - 1],
                send_sem=send_sem.at[k - 1],
                recv_sem=recv_sem.at[k - 1],
                device_id=peer(at),
                device_id_type=pl.DeviceIdType.MESH,
            )

        barrier = pltpu.get_barrier_semaphore()

        @pl.loop(1, n)
        def _(k):
            pl.semaphore_signal(
                barrier,
                inc=1,
                device_id=peer(lax.rem(me + k, n)),
                device_id_type=pl.DeviceIdType.MESH,
            )

        pl.semaphore_wait(barrier, n - 1)

        @pl.loop(1, n)
        def _(k):
            copy(k).start()

        @pl.loop(1, n)
        def _(k):
            copy(k).wait()

        @pl.loop(0, rows // step)
        def _(i):
            span = pl.ds(pl.multiple_of(i * step, step), step)
            own = x_ref[me, span, :] if split else x_ref[span, :]
            total = own.astype(jnp.float32)
            for k in range(n - 1):
                total = total + landed[k, span, :].astype(jnp.float32)
            o_ref[span, :] = total.astype(o_ref.dtype)

    return pl.pallas_call(
        kernel,
        out_shape=jax.ShapeDtypeStruct((rows, cols), x.dtype),
        in_specs=[pl.BlockSpec(memory_space=pltpu.VMEM)],
        out_specs=pl.BlockSpec(memory_space=pltpu.VMEM),
        scratch_shapes=[
            pltpu.VMEM((n - 1, rows, cols), x.dtype),
            pltpu.SemaphoreType.DMA((n - 1,)),
            pltpu.SemaphoreType.DMA((n - 1,)),
        ],
        compiler_params=pltpu.CompilerParams(collective_id=collective_id, has_side_effects=True),
    )(x)


def on_group(stride, n):
    def place():
        g, s = lax.axis_index("group"), lax.axis_index("shard")
        digit = lax.rem(g // stride, n)
        return digit, lambda at: (g + (at - digit) * stride, s)

    return place


def on_shard():
    g, s = lax.axis_index("group"), lax.axis_index("shard")
    return s, lambda at: (g, at)


def on_all():
    width = lax.axis_size("shard")
    g, s = lax.axis_index("group"), lax.axis_index("shard")
    return g * width + s, lambda at: (at // width, lax.rem(at, width))


def scatter_over_group(x, first_id):
    groups = lax.axis_size("group")
    local, rows, cols = x.shape[0] // groups, x.shape[1], x.shape[2]
    pairs = x.reshape(groups // 2, 2, local * rows, cols).transpose(1, 0, 2, 3)
    pairs = pairs.reshape(2, groups // 2 * local * rows, cols)
    half = exchange_sum(pairs, on_group(1, 2), 2, True, first_id)
    half = half.reshape(groups // 2, local * rows, cols)
    out = exchange_sum(half, on_group(2, groups // 2), groups // 2, True, first_id + 1)
    return out.reshape(local, rows, cols)


def shards(momentum, gradient, q_prev, owner_group, group_counts):
    me = lax.axis_index("group")
    experts, block, hidden = momentum.shape
    cap, share_rows, rank = q_prev.shape[1:]
    slot_of = owner_slots(owner_group)
    keep = slot_of < group_counts[owner_group]
    mine = keep & (owner_group == me)

    pieces = jnp.zeros((experts, share_rows, rank), jnp.bfloat16)
    for j in range(cap):
        pick = mine & (slot_of == j)
        pieces = jnp.where(pick[:, None, None], q_prev[0, j][None], pieces)
    q_one = scatter_over_group(pieces, 0)
    q_shard = lax.all_gather(q_one, "shard", axis=1, tiled=True)
    q_full = lax.all_gather(q_shard, "group", axis=0, tiled=True)

    combined = (momentum.astype(jnp.float32) + gradient.astype(jnp.float32)).astype(jnp.bfloat16)
    left_raw = jnp.einsum("erh,ehk->erk", combined, q_full, preferred_element_type=jnp.float32)
    devices = lax.axis_size("group") * lax.axis_size("shard")
    squares = exchange_sum(jnp.sum(left_raw * left_raw, axis=1), on_all, devices, False, 2)
    left_unit = (left_raw * lax.rsqrt(squares + stability_offset)[:, None, :]).astype(jnp.bfloat16)
    part = jnp.einsum("erh,erk->ehk", combined, left_unit, preferred_element_type=jnp.float32)

    part = scatter_over_group(part.astype(jnp.bfloat16), 3)
    ring = lax.axis_size("shard")
    local = part.shape[0]
    part = part.reshape(local, ring, share_rows, rank).transpose(1, 0, 2, 3)
    part = part.reshape(ring, local * share_rows, rank)
    share = exchange_sum(part, on_shard, ring, True, 5).reshape(local, share_rows, rank)
    right = lax.all_gather(share, "shard", axis=1, tiled=True)
    right = lax.all_gather(right, "group", axis=0, tiled=True)

    right32 = right.astype(jnp.float32)
    scale = lax.rsqrt(jnp.mean(right32 * right32, axis=1) + stability_offset)
    q_new = (right32 * scale[:, None, :]).astype(jnp.bfloat16)
    update = (
        jnp.einsum("erk,ehk->erh", left_unit, q_new, preferred_element_type=jnp.float32)
        * math.sqrt(D / RANK)
    ).astype(jnp.bfloat16)
    low_rank = jnp.einsum("erk,ehk->erh", left_unit, right, preferred_element_type=jnp.float32)
    momentum_next = (
        combined.astype(jnp.float32) - (1.0 - momentum_decay) * low_rank
    ).astype(jnp.bfloat16)

    rows = lax.dynamic_slice_in_dim(q_new, lax.axis_index("shard") * share_rows, share_rows, axis=1)
    kept = []
    for j in range(cap):
        pick = mine & (slot_of == j)
        kept.append(jnp.sum(jnp.where(pick[:, None, None], rows, jnp.zeros_like(rows)), axis=0))
    return (momentum_next, update, jnp.stack(kept)[None])


def solution(mesh):
    return jax.shard_map(
        shards,
        mesh=mesh,
        in_specs=(
            P(None, AXES, None),
            P(None, AXES, None),
            P("group", None, "shard", None),
            P(),
            P(),
        ),
        out_specs=(P(None, AXES, None), P(None, AXES, None), P("group", None, "shard", None)),
        check_vma=False,
    )
```
